32 devices in a mesh: row: 4 (over z), col: 8 (over y, x, core).
Axes of the slice: x: 2, y: 2, z: 4, core: 2. Of those that a mesh axis runs over, the one named last changes fastest.
Arguments:
- tokens: bfloat16 [24576, 256], P(('row', 'col'))
- codebook: bfloat16 [16384, 256], P(('row', 'col')), may hold values from -6 to 6
- codes: int32 [24576], P(('row', 'col')), may hold values from 0 to 16383
Outputs:
- quantized: bfloat16 [24576, 256], P(('row', 'col'))
- token_loss: float32 [24576], P(('row', 'col'))
- code_counts: int32 [16384], P(('row', 'col'))
- code_loss: float32 [16384], P(('row', 'col'))
- commitment: float32 [], replicated
- perplexity: float32 [], replicated
The draws below stay inside these ranges and needn't reach their ends.
All inputs are finite; a program needn't handle non-finite values.
Results may differ from the reference program's by a relative error of at most 0.0004.
Values may be sent and summed in bfloat16 or wider, within the bound.
No kernel may reach another device: no remote copies, remote signals or barrier semaphores. Data moves between devices by JAX's collectives and lax.ppermute only.
A program may use at most 64 MiB of HBM per device.

```python
import math
import jax
import jax.numpy as jnp
import numpy as np

DIM = 256
CODES = 16384
TOKENS = 24576


def draw_tokens(key, part):
    key_norm = jax.random.fold_in(key, 11)
    key_scale = jax.random.fold_in(key, 12)
    values = jax.random.normal(key_norm, (TOKENS, DIM), jnp.float32)
    spread = jnp.exp(jax.random.uniform(key_scale, (TOKENS, 1), jnp.float32, jnp.log(0.2), jnp.log(2.0)))
    rising = 1.0 + 2.0 * jnp.arange(TOKENS, dtype=jnp.float32)[:, None] / TOKENS
    return (values * spread * rising).astype(jnp.bfloat16)


def touch_ends(drawn, own_key, smallest, top_value):
    index_at = [jax.random.randint(jax.random.fold_in(own_key, axis), (), 0, length) for axis, length in enumerate(drawn.shape)]
    main_axis = drawn.shape.index(max(drawn.shape))
    next_to = index_at[:main_axis] + [(index_at[main_axis] + 1) % drawn.shape[main_axis]] + index_at[main_axis + 1:]
    return drawn.at[tuple(index_at)].set(smallest).at[tuple(next_to)].set(top_value)


def levels(rng, extent, cuts, low, top_value):
    def one(position, shards_of):
        draws = jax.random.uniform(jax.random.fold_in(jax.random.fold_in(rng, 6), position), (shards_of,), jnp.float32, low / len(cuts), top_value / len(cuts))
        return jnp.repeat(jnp.exp(draws), extent[position] // shards_of).reshape((-1,) + (1,) * (len(extent) - position - 1))

    level = one(*cuts[0])
    for cut in cuts[1:]:
        level = level * one(*cut)
    return level


def rank_bounds(amount, lean):
    portions = [(1 << 20) // math.isqrt(rank ** lean) + 1 for rank in range(1, amount + 1)]
    scale = 1 + sum(portions) // (1 << 30)
    return np.cumsum(np.array([max(1, weight // scale) for weight in portions]))


def ranked(own_key, extent, count, lean):
    listing = rank_bounds(count, lean)
    lot = jax.random.randint(jax.random.fold_in(own_key, 1), extent, 0, int(listing[count - 1]))
    rank = jnp.searchsorted(jnp.asarray(listing, jnp.int32), lot, side="right")
    return jax.random.permutation(jax.random.fold_in(own_key, 2), count)[rank].astype(jnp.int32)


def normal_values(stream_key, shape, scale, most, cuts=(), kind=jnp.bfloat16):
    loudness = levels(stream_key, shape, cuts, -0.22, 0.18) if cuts else 1.0
    entries = jax.random.normal(stream_key, shape, jnp.float32) * scale * loudness
    return jnp.minimum(jnp.maximum(entries, -most), most).astype(kind)


def setup_inputs(seed: int = 0) -> dict:
    seeds = jax.random.split(jax.random.key(seed), 4)
    tokens = draw_tokens(jax.random.fold_in(seeds[3], 71), 0)
    codebook = normal_values(seeds[1], (CODES, DIM), 1.0, 6.0, ((0, 32),))
    codes = touch_ends(ranked(seeds[2], (TOKENS,), CODES, 2), jax.random.fold_in(seeds[2], 3), 0, CODES - 1).astype(jnp.int32)
    return dict(tokens=tokens, codebook=codebook, codes=codes)


def reference(tokens, codebook, codes):
    quantized = jnp.take(codebook, codes, axis=0)
    diff = tokens.astype(jnp.float32) - quantized.astype(jnp.float32)
    token_loss = jnp.sum(diff * diff, axis=1) / DIM
    code_counts = jnp.zeros((CODES,), jnp.int32).at[codes].add(1)
    code_loss = jax.ops.segment_sum(token_loss, codes, num_segments=CODES)
    commitment = 0.25 * jnp.sum(token_loss) / TOKENS
    probs = code_counts.astype(jnp.float32) / TOKENS
    floor_prob = jnp.float32(1.0 / TOKENS)
    terms = jnp.where(code_counts > 0, probs * jnp.log(jnp.maximum(probs, floor_prob)), jnp.float32(0.0))
    perplexity = jnp.exp(-jnp.sum(terms))
    return quantized, token_loss, code_counts, code_loss, commitment, perplexity
```

```python
import functools

import jax
import jax.numpy as jnp
from jax import lax
from jax.experimental import pallas as pl
from jax.experimental.pallas import tpu as pltpu
from jax.sharding import PartitionSpec as P

AXES = ("row", "col")
LANES = 128
SLOTS = 32
F32 = jnp.float32
BF16 = jnp.bfloat16
VMEM = pl.BlockSpec(memory_space=pltpu.VMEM)
SMEM = pl.BlockSpec(memory_space=pltpu.SMEM)


def iota(shape, dim):
    return lax.broadcasted_iota(jnp.int32, shape, dim)


def ones_where(mask):
    return jnp.where(mask, F32(1.0), F32(0.0)).astype(BF16)


def dot(a, b, dims=((1,), (0,))):
    return lax.dot_general(a, b, (dims, ((), ())), preferred_element_type=F32)


def rank_within(present):
    width = present.shape[1]
    before = ones_where(iota((width, width), 0) < iota((width, width), 1))
    return dot(ones_where(present), before)


def rows_equal(ids, count):
    steps = iota((count, LANES), 0)
    return jnp.concatenate(
        [steps == ids[k : k + 1, :] for k in range(ids.shape[0])], axis=1
    )


def request_kernel(codes_ref, pay_ref, slot_ref, *, devices, per_dev, slots):
    codes = codes_ref[...]
    shift = per_dev.bit_length() - 1
    owner_mask = rows_equal(codes >> shift, devices)
    local = ones_where(rows_equal(codes & (per_dev - 1), per_dev))
    hist = dot(ones_where(owner_mask), local, ((1,), (1,)))
    present = hist > 0.5
    rank = rank_within(present)
    unique = jnp.sum(jnp.where(present, F32(1.0), F32(0.0)), axis=1, keepdims=True)
    most = jnp.max(unique, axis=0, keepdims=True)
    pay_ref[:, :LANES] = jnp.broadcast_to(most, (devices, LANES))
    pay_ref[:, LANES:] = hist
    capped = jnp.minimum(rank, F32(slots - 1)).astype(BF16)
    per_token = dot(capped, local)
    base = (iota(owner_mask.shape, 0) * slots).astype(F32)
    slot = jnp.sum(
        jnp.where(owner_mask, per_token + base, F32(0.0)), axis=0, keepdims=True
    )
    slot_ref[...] = jnp.zeros(slot_ref.shape, F32)
    for k in range(codes.shape[0]):
        slot_ref[k : k + 1, :] = slot[:, k * LANES : (k + 1) * LANES]


def serve_kernel(pay_ref, book_ref, send_ref, rank_ref, counts_ref, ent_ref, most_ref, *, slots, total_tokens):
    devices = pay_ref.shape[0]
    per_dev = book_ref.shape[0]
    hist = pay_ref[:, LANES:]
    most_ref[0, 0] = jnp.max(pay_ref[:, :LANES])
    present = hist > 0.5
    rank_ref[...] = jnp.where(present, rank_within(present), F32(-1.0))
    counts = jnp.sum(hist, axis=0, keepdims=True)
    counts_ref[...] = counts.astype(jnp.int32)
    probs = counts / total_tokens
    terms = jnp.where(
        counts > 0.5,
        probs * jnp.log(jnp.maximum(probs, F32(1.0 / total_tokens))),
        F32(0.0),
    )
    ent_ref[...] = jnp.broadcast_to(jnp.sum(terms, axis=1, keepdims=True), ent_ref.shape)
    book = book_ref[...]
    steps = iota((slots, per_dev), 0).astype(F32)

    def group(g, carry):
        ranks = rank_ref[pl.ds(pl.multiple_of(g * 8, 8), 8), :]
        pick = jnp.concatenate(
            [ones_where(steps == ranks[j : j + 1, :]) for j in range(8)], axis=0
        )
        rows = dot(pick, book).astype(BF16)
        send_ref[pl.ds(pl.multiple_of(g * 8 * slots, 8 * slots), 8 * slots), :] = rows
        return carry

    lax.fori_loop(0, devices // 8, group, 0)


def loss_kernel(slot_ref, tokens_ref, recv_ref, ent_ref, quant_ref, loss_ref, back_ref, *, slots, block):
    tok_rows, width = tokens_ref.shape
    chunks = tok_rows // LANES
    devices = back_ref.shape[0]
    slot = slot_ref[...]
    cols = slot.T
    steps = iota((LANES, block), 1).astype(F32)

    def gather(b, acc):
        first = (b * block).astype(F32) if recv_ref.shape[0] > block else F32(0.0)
        pick = jnp.concatenate(
            [ones_where(steps == cols[:, k : k + 1] - first) for k in range(chunks)],
            axis=0,
        )
        start = pl.multiple_of(b * block, block)
        return acc + dot(pick, recv_ref[pl.ds(start, block), :])

    steps_n = recv_ref.shape[0] // block
    if steps_n == 1:
        pick = jnp.concatenate(
            [ones_where(steps == cols[:, k : k + 1]) for k in range(chunks)], axis=0
        )
        quant = dot(pick, recv_ref[...])
    else:
        quant = lax.fori_loop(0, steps_n, gather, jnp.zeros((tok_rows, width), F32))
    quant_ref[...] = quant.astype(BF16)
    diff = tokens_ref[...].astype(F32) - quant
    loss = jnp.sum(diff * diff, axis=1, keepdims=True) / width
    total = jnp.sum(loss, axis=0, keepdims=True)
    rows = []
    for k in range(chunks):
        part = jnp.broadcast_to(loss[k * LANES : (k + 1) * LANES, :], (LANES, LANES))
        row = part.T[0:1, :]
        loss_ref[k : k + 1, :] = row
        rows.append(row)
    loss_row = jnp.concatenate(rows, axis=1)
    slot_int = slot.astype(jnp.int32)[:chunks]
    shift = slots.bit_length() - 1
    owner_mask = rows_equal(slot_int >> shift, devices)
    rank = ones_where(rows_equal(slot_int & (slots - 1), LANES))
    high = loss_row.astype(BF16).astype(F32)
    mid = (loss_row - high).astype(BF16).astype(F32)
    low = loss_row - high - mid
    sums = jnp.zeros((devices, LANES), F32)
    for piece in (low, mid, high):
        weighted = jnp.where(owner_mask, piece, F32(0.0)).astype(BF16)
        sums = sums + dot(weighted, rank, ((1,), (1,)))
    lane = iota((devices, LANES), 1)
    ent = jnp.broadcast_to(ent_ref[...], (devices, LANES))
    back_ref[...] = jnp.where(
        lane == slots, total, jnp.where(lane == slots + 1, ent, sums)
    )


def collect_kernel(back_ref, rank_ref, code_loss_ref, commit_ref, perp_ref, *, slots, total_tokens):
    devices, per_dev = rank_ref.shape

    def group(g, acc):
        at = pl.ds(pl.multiple_of(g * 8, 8), 8)
        ranks = rank_ref[at, :]
        back = back_ref[at, :]
        for r in range(slots):
            acc = acc + jnp.where(ranks == F32(r), back[:, r : r + 1], F32(0.0))
        return acc

    acc = lax.fori_loop(0, devices // 8, group, jnp.zeros((8, per_dev), F32))
    code_loss_ref[...] = jnp.sum(acc, axis=0, keepdims=True)
    sums = jnp.sum(back_ref[...], axis=0, keepdims=True)
    commit_ref[...] = 0.25 * sums[:, slots : slots + 1] / total_tokens
    perp_ref[...] = jnp.exp(-sums[:, slots + 1 : slots + 2])


def on_device(tokens, codebook, codes, *, devices):
    tok_rows, width = tokens.shape
    per_dev = codebook.shape[0]
    total_tokens = tok_rows * devices
    slots = min(SLOTS, per_dev)
    chunks = tok_rows // LANES
    n_slots = devices * slots
    shape = jax.ShapeDtypeStruct

    pay, slot = pl.pallas_call(
        functools.partial(request_kernel, devices=devices, per_dev=per_dev, slots=slots),
        out_shape=(
            shape((devices, LANES + per_dev), F32),
            shape((-(-chunks // 8) * 8, LANES), F32),
        ),
        in_specs=[VMEM],
        out_specs=(VMEM, VMEM),
        name="request",
    )(codes.reshape(chunks, LANES))
    pay_in = lax.all_to_all(pay, AXES, 0, 0, tiled=True)
    send, rank, counts, ent, most = pl.pallas_call(
        functools.partial(serve_kernel, slots=slots, total_tokens=total_tokens),
        out_shape=(
            shape((n_slots, width), BF16),
            shape((devices, per_dev), F32),
            shape((1, per_dev), jnp.int32),
            shape((1, LANES), F32),
            shape((1, 1), F32),
        ),
        in_specs=[VMEM, VMEM],
        out_specs=(VMEM, VMEM, VMEM, VMEM, SMEM),
        name="serve",
    )(pay_in, codebook)
    code_counts = counts.reshape(per_dev)

    def exchange_slots(tokens, codebook, codes, slot, send, rank, ent):
        recv = lax.all_to_all(send, AXES, 0, 0, tiled=True)
        quantized, loss, back = pl.pallas_call(
            functools.partial(loss_kernel, slots=slots, block=min(n_slots, 1024)),
            out_shape=(
                shape((tok_rows, width), BF16),
                shape((chunks, LANES), F32),
                shape((devices, LANES), F32),
            ),
            in_specs=[VMEM] * 4,
            out_specs=(VMEM,) * 3,
            name="losses",
        )(slot, tokens, recv, ent)
        back_in = lax.all_to_all(back, AXES, 0, 0, tiled=True)
        code_loss, commit, perp = pl.pallas_call(
            functools.partial(collect_kernel, slots=slots, total_tokens=total_tokens),
            out_shape=(shape((1, per_dev), F32), shape((1, 1), F32), shape((1, 1), F32)),
            in_specs=[VMEM] * 2,
            out_specs=(VMEM,) * 3,
            name="collect",
        )(back_in, rank)
        return (
            quantized,
            loss.reshape(tok_rows),
            code_loss.reshape(per_dev),
            commit.reshape(()),
            perp.reshape(()),
        )

    def exchange_book(tokens, codebook, codes, slot, send, rank, ent):
        spread = jnp.broadcast_to(codebook[None], (devices, per_dev, width))
        book = lax.all_to_all(spread, AXES, 0, 0, tiled=True)
        book = book.reshape(devices * per_dev, width)
        quantized = jnp.take(book, codes, axis=0, mode="clip")
        diff = tokens.astype(F32) - quantized.astype(F32)
        token_loss = jnp.sum(diff * diff, axis=1) / width
        part = jax.ops.segment_sum(token_loss, codes, num_segments=devices * per_dev)
        part = lax.all_to_all(part.reshape(devices, per_dev), AXES, 0, 0, tiled=True)
        lane = iota((devices, LANES), 1)
        pair = jnp.where(lane == 0, jnp.sum(token_loss), ent)
        sums = jnp.sum(lax.all_to_all(pair, AXES, 0, 0, tiled=True), axis=0)
        return (
            quantized,
            token_loss,
            jnp.sum(part, axis=0),
            0.25 * sums[0] / total_tokens,
            jnp.exp(-sums[1]),
        )

    quantized, token_loss, code_loss, commitment, perplexity = lax.cond(
        most[0, 0] > slots,
        exchange_book,
        exchange_slots,
        tokens, codebook, codes, slot, send, rank, ent,
    )
    return (quantized, token_loss, code_counts, code_loss, commitment, perplexity)


def solution(mesh):
    devices = mesh.shape["row"] * mesh.shape["col"]
    split = P(AXES)
    return jax.shard_map(
        functools.partial(on_device, devices=devices),
        mesh=mesh,
        in_specs=(P(AXES, None), P(AXES, None), split),
        out_specs=(P(AXES, None), split, split, split, P(), P()),
        check_vma=False,
    )
```

```python
import functools

import jax
import jax.numpy as jnp
from jax import lax
from jax.experimental import pallas as pl
from jax.experimental.pallas import tpu as pltpu
from jax.sharding import PartitionSpec as P

AXES = ("row", "col")
LANES = 128
SLOTS = 32
F32 = jnp.float32
BF16 = jnp.bfloat16
VMEM = pl.BlockSpec(memory_space=pltpu.VMEM)
ANY = pl.BlockSpec(memory_space=pl.ANY)
SMEM = pl.BlockSpec(memory_space=pltpu.SMEM)


def iota(shape, dim):
    return lax.broadcasted_iota(jnp.int32, shape, dim)


def ones_where(mask):
    return jnp.where(mask, F32(1.0), F32(0.0)).astype(BF16)


def dot(a, b, dims=((1,), (0,))):
    return lax.dot_general(a, b, (dims, ((), ())), preferred_element_type=F32)


def rank_within(present):
    width = present.shape[1]
    before = ones_where(iota((width, width), 0) < iota((width, width), 1))
    return dot(ones_where(present), before)


def rows_equal(ids, count):
    steps = iota((count, LANES), 0)
    return jnp.concatenate(
        [steps == ids[k : k + 1, :] for k in range(ids.shape[0])], axis=1
    )


def request_kernel(codes_ref, tokens_ref, pay_ref, slot_ref, near_tokens_ref, sem, *, devices, per_dev, slots):
    fetch_tokens = pltpu.make_async_copy(tokens_ref, near_tokens_ref, sem)
    fetch_tokens.start()
    codes = codes_ref[...]
    shift = per_dev.bit_length() - 1
    tiles = pay_ref.shape[0] // devices
    owner_mask = rows_equal(codes >> shift, devices)
    local = ones_where(rows_equal(codes & (per_dev - 1), tiles * LANES))
    hist = dot(ones_where(owner_mask), local, ((1,), (1,)))
    present = hist > 0.5
    rank = rank_within(present)
    unique = jnp.sum(jnp.where(present, F32(1.0), F32(0.0)), axis=1, keepdims=True)
    most = jnp.max(unique, axis=0, keepdims=True)
    coded = jnp.where(most > F32(slots), -1.0 - hist, hist)
    for j in range(tiles):
        pay_ref[pl.ds(j, devices, stride=tiles), :] = coded[:, j * LANES : (j + 1) * LANES]
    capped = jnp.minimum(rank, F32(slots - 1)).astype(BF16)
    per_token = dot(capped, local)
    base = (iota(owner_mask.shape, 0) * slots).astype(F32)
    slot = jnp.sum(
        jnp.where(owner_mask, per_token + base, F32(0.0)), axis=0, keepdims=True
    )
    slot_ref[...] = jnp.zeros(slot_ref.shape, F32)
    for k in range(codes.shape[0]):
        slot_ref[k : k + 1, :] = slot[:, k * LANES : (k + 1) * LANES]
    fetch_tokens.wait()


def serve_kernel(pay_ref, book_ref, send_ref, rank_ref, counts_ref, ent_ref, least_ref, near_ref, sem, *, slots, total_tokens):
    fetch = pltpu.make_async_copy(book_ref, near_ref, sem)
    fetch.start()
    devices = rank_ref.shape[0]
    per_dev = book_ref.shape[0]
    tiles = pay_ref.shape[0] // devices
    coded = jnp.concatenate(
        [pay_ref[pl.ds(j, devices, stride=tiles), :] for j in range(tiles)], axis=1
    )[:, :per_dev]
    least_ref[0, 0] = jnp.min(coded)
    hist = jnp.where(coded < 0.0, -1.0 - coded, coded)
    present = hist > 0.5
    rank_ref[...] = jnp.where(present, rank_within(present), F32(-1.0))
    counts = jnp.sum(hist, axis=0, keepdims=True)
    counts_ref[...] = counts.astype(jnp.int32)
    probs = counts / total_tokens
    terms = jnp.where(
        counts > 0.5,
        probs * jnp.log(jnp.maximum(probs, F32(1.0 / total_tokens))),
        F32(0.0),
    )
    ent_ref[...] = jnp.broadcast_to(jnp.sum(terms, axis=1, keepdims=True), ent_ref.shape)
    fetch.wait()
    book = near_ref[...]
    steps = iota((slots, per_dev), 0).astype(F32)

    def group(g, carry):
        ranks = rank_ref[pl.ds(pl.multiple_of(g * 8, 8), 8), :]
        pick = jnp.concatenate(
            [ones_where(steps == ranks[j : j + 1, :]) for j in range(8)], axis=0
        )
        rows = dot(pick, book).astype(BF16)
        send_ref[pl.ds(pl.multiple_of(g * 8 * slots, 8 * slots), 8 * slots), :] = rows
        return carry

    lax.fori_loop(0, devices // 8, group, 0)


def loss_kernel(slot_ref, tokens_ref, recv_ref, ent_ref, quant_ref, loss_ref, back_ref, near_ref, sems, *, slots, block):
    tok_rows, width = tokens_ref.shape
    chunks = tok_rows // LANES
    devices = back_ref.shape[0]
    slot = slot_ref[...]
    cols = slot.T
    steps = iota((LANES, block), 1).astype(F32)
    copies = []
    rows = []
    for k in range(chunks):
        at = pl.ds(k * LANES, LANES)
        col = cols[:, k : k + 1]
        if recv_ref.shape[0] == block:
            quant = dot(ones_where(steps == col), recv_ref[...])
        else:

            def gather(b, acc):
                start = pl.multiple_of(b * block, block)
                pick = ones_where(steps == col - (b * block).astype(F32))
                return acc + dot(pick, recv_ref[pl.ds(start, block), :])

            quant = lax.fori_loop(
                0, recv_ref.shape[0] // block, gather, jnp.zeros((LANES, width), F32)
            )
        near_ref[at, :] = quant.astype(BF16)
        copy = pltpu.make_async_copy(near_ref.at[at, :], quant_ref.at[at, :], sems.at[k])
        copy.start()
        copies.append(copy)
        diff = tokens_ref[at, :].astype(F32) - quant
        loss = jnp.sum(diff * diff, axis=1, keepdims=True) / width
        row = jnp.broadcast_to(loss, (LANES, LANES)).T[0:1, :]
        loss_ref[k : k + 1, :] = row
        rows.append(row)
    loss_row = jnp.concatenate(rows, axis=1)
    total = jnp.sum(loss_row, axis=1, keepdims=True)
    slot_int = slot.astype(jnp.int32)[:chunks]
    shift = slots.bit_length() - 1
    owner_mask = rows_equal(slot_int >> shift, devices)
    rank = ones_where(rows_equal(slot_int & (slots - 1), LANES))
    high = loss_row.astype(BF16).astype(F32)
    mid = (loss_row - high).astype(BF16).astype(F32)
    low = loss_row - high - mid
    weighted = jnp.concatenate(
        [jnp.where(owner_mask, p, F32(0.0)).astype(BF16) for p in (low, mid, high)],
        axis=1,
    )
    sums = dot(weighted, jnp.concatenate([rank] * 3, axis=1), ((1,), (1,)))
    lane = iota((devices, LANES), 1)
    ent = jnp.broadcast_to(ent_ref[...], (devices, LANES))
    back_ref[...] = jnp.where(
        lane == slots, total, jnp.where(lane == slots + 1, ent, sums)
    )
    for copy in copies:
        copy.wait()


def collect_kernel(back_ref, rank_ref, code_loss_ref, commit_ref, perp_ref, *, slots, total_tokens):
    devices, per_dev = rank_ref.shape

    def group(g, acc):
        at = pl.ds(pl.multiple_of(g * 8, 8), 8)
        ranks = rank_ref[at, :]
        back = back_ref[at, :]
        parts = [acc] + [jnp.zeros_like(acc)] * 3
        for r in range(slots):
            term = jnp.where(ranks == F32(r), back[:, r : r + 1], F32(0.0))
            parts[r % 4] = parts[r % 4] + term
        return (parts[0] + parts[1]) + (parts[2] + parts[3])

    acc = lax.fori_loop(0, devices // 8, group, jnp.zeros((8, per_dev), F32))
    code_loss = jnp.sum(acc, axis=0, keepdims=True)
    lanes = code_loss_ref.shape[1]
    for j in range(code_loss_ref.shape[0]):
        code_loss_ref[j : j + 1, :] = code_loss[:, j * lanes : (j + 1) * lanes]
    sums = jnp.sum(back_ref[...], axis=0, keepdims=True)
    commit_ref[...] = 0.25 * sums[:, slots : slots + 1] / total_tokens
    perp_ref[...] = jnp.exp(-sums[:, slots + 1 : slots + 2])


def on_device(tokens, codebook, codes, *, devices):
    tok_rows, width = tokens.shape
    per_dev = codebook.shape[0]
    total_tokens = tok_rows * devices
    slots = min(SLOTS, per_dev)
    chunks = tok_rows // LANES
    n_slots = devices * slots
    shape = jax.ShapeDtypeStruct

    tiles = max(per_dev // LANES, 1)
    pay, slot, near_tokens = pl.pallas_call(
        functools.partial(request_kernel, devices=devices, per_dev=per_dev, slots=slots),
        out_shape=(
            shape((devices * tiles, LANES), F32),
            shape((-(-chunks // 8) * 8, LANES), F32),
            shape(tokens.shape, BF16),
        ),
        in_specs=[VMEM, ANY],
        out_specs=(VMEM,) * 3,
        scratch_shapes=[pltpu.SemaphoreType.DMA],
        name="request",
    )(codes.reshape(chunks, LANES), tokens)
    pay_in = lax.all_to_all(pay.reshape(devices, tiles, LANES), AXES, 0, 0)
    pay_in = pay_in.reshape(devices * tiles, LANES)
    send, rank, counts, ent, least = pl.pallas_call(
        functools.partial(serve_kernel, slots=slots, total_tokens=total_tokens),
        out_shape=(
            shape((n_slots, width), BF16),
            shape((devices, per_dev), F32),
            shape((1, per_dev), jnp.int32),
            shape((1, LANES), F32),
            shape((1, 1), F32),
        ),
        in_specs=[VMEM, ANY],
        out_specs=(VMEM, VMEM, VMEM, VMEM, SMEM),
        scratch_shapes=[pltpu.VMEM(codebook.shape, BF16), pltpu.SemaphoreType.DMA],
        name="serve",
    )(pay_in, codebook)
    code_counts = counts.reshape(per_dev)

    def exchange_slots(tokens, near_tokens, codebook, codes, slot, send, rank, ent):
        recv = lax.all_to_all(send, AXES, 0, 0, tiled=True)
        quantized, loss, back = pl.pallas_call(
            functools.partial(loss_kernel, slots=slots, block=min(n_slots, 1024)),
            out_shape=(
                shape((tok_rows, width), BF16),
                shape((chunks, LANES), F32),
                shape((devices, LANES), F32),
            ),
            in_specs=[VMEM] * 4,
            out_specs=(ANY, VMEM, VMEM),
            scratch_shapes=[
                pltpu.VMEM((tok_rows, width), BF16),
                pltpu.SemaphoreType.DMA((chunks,)),
            ],
            name="losses",
        )(slot, near_tokens, recv, ent)
        back_in = lax.all_to_all(back, AXES, 0, 0, tiled=True)
        code_loss, commit, perp = pl.pallas_call(
            functools.partial(collect_kernel, slots=slots, total_tokens=total_tokens),
            out_shape=(shape((tiles, per_dev // tiles), F32), shape((1, 1), F32), shape((1, 1), F32)),
            in_specs=[VMEM] * 2,
            out_specs=(VMEM,) * 3,
            name="collect",
        )(back_in, rank)
        return (
            quantized,
            loss.reshape(tok_rows),
            code_loss.reshape(per_dev),
            commit.reshape(()),
            perp.reshape(()),
        )

    def exchange_book(tokens, near_tokens, codebook, codes, slot, send, rank, ent):
        spread = jnp.broadcast_to(codebook[None], (devices, per_dev, width))
        book = lax.all_to_all(spread, AXES, 0, 0, tiled=True)
        book = book.reshape(devices * per_dev, width)
        quantized = jnp.take(book, codes, axis=0, mode="clip")
        diff = tokens.astype(F32) - quantized.astype(F32)
        token_loss = jnp.sum(diff * diff, axis=1) / width
        part = jax.ops.segment_sum(token_loss, codes, num_segments=devices * per_dev)
        part = lax.all_to_all(part.reshape(devices, per_dev), AXES, 0, 0, tiled=True)
        lane = iota((devices, LANES), 1)
        pair = jnp.where(lane == 0, jnp.sum(token_loss), ent)
        sums = jnp.sum(lax.all_to_all(pair, AXES, 0, 0, tiled=True), axis=0)
        return (
            quantized,
            token_loss,
            jnp.sum(part, axis=0),
            0.25 * sums[0] / total_tokens,
            jnp.exp(-sums[1]),
        )

    quantized, token_loss, code_loss, commitment, perplexity = lax.cond(
        least[0, 0] < 0.0,
        exchange_book,
        exchange_slots,
        tokens, near_tokens, codebook, codes, slot, send, rank, ent,
    )
    return (quantized, token_loss, code_counts, code_loss, commitment, perplexity)


def solution(mesh):
    devices = mesh.shape["row"] * mesh.shape["col"]
    split = P(AXES)
    return jax.shard_map(
        functools.partial(on_device, devices=devices),
        mesh=mesh,
        in_specs=(P(AXES, None), P(AXES, None), split),
        out_specs=(P(AXES, None), split, split, split, P(), P()),
        check_vma=False,
    )
```

```python
import functools

import jax
import jax.numpy as jnp
from jax import lax
from jax.experimental import pallas as pl
from jax.experimental.pallas import tpu as pltpu
from jax.sharding import PartitionSpec as P

AXES = ("row", "col")
LANES = 128
SLOTS = 32
F32 = jnp.float32
BF16 = jnp.bfloat16
VMEM = pl.BlockSpec(memory_space=pltpu.VMEM)
ANY = pl.BlockSpec(memory_space=pl.ANY)
SMEM = pl.BlockSpec(memory_space=pltpu.SMEM)


def iota(shape, dim):
    return lax.broadcasted_iota(jnp.int32, shape, dim)


def ones_where(mask):
    return jnp.where(mask, F32(1.0), F32(0.0)).astype(BF16)


def dot(a, b, dims=((1,), (0,))):
    return lax.dot_general(a, b, (dims, ((), ())), preferred_element_type=F32)


def fold(x, rows):
    while x.shape[0] > rows:
        half = x.shape[0] // 2
        x = x[:half] + x[half:]
    return x


def rank_within(present, tiles):
    ones = ones_where(present)
    lane = (LANES, LANES)
    rank = dot(ones, ones_where(iota(lane, 0) < iota(lane, 1)))
    unique = jnp.sum(jnp.where(present, F32(1.0), F32(0.0)), axis=1, keepdims=True)
    row = iota(unique.shape, 0) & (tiles - 1)
    earlier = jnp.zeros_like(unique)
    for j in range(1, tiles):
        moved = pltpu.roll(jnp.broadcast_to(unique, present.shape), j, 0)[:, :1]
        earlier = earlier + jnp.where(row >= j, moved, F32(0.0))
    return rank + earlier, unique + earlier


def rows_equal(ids, count):
    steps = iota((count, LANES), 0)
    return jnp.concatenate(
        [steps == ids[k : k + 1, :] for k in range(ids.shape[0])], axis=1
    )


def request_kernel(codes_ref, tokens_ref, pay_ref, slot_ref, near_tokens_ref, sem, *, devices, per_dev, slots):
    fetch_tokens = pltpu.make_async_copy(tokens_ref, near_tokens_ref, sem)
    fetch_tokens.start()
    codes = codes_ref[...]
    tiles = pay_ref.shape[0] // devices
    span = per_dev // tiles
    row_mask = rows_equal(codes >> (span.bit_length() - 1), devices * tiles)
    lanes = ones_where(rows_equal(codes & (span - 1), LANES))
    hist = dot(ones_where(row_mask), lanes, ((1,), (1,)))
    rank, unique = rank_within(hist > 0.5, tiles)
    most = jnp.max(unique, axis=0, keepdims=True)
    pay_ref[...] = jnp.where(most > F32(slots), -1.0 - hist, hist)
    capped = jnp.minimum(rank, F32(slots - 1)).astype(BF16)
    per_token = dot(capped, lanes)
    owner = iota(row_mask.shape, 0) >> (tiles.bit_length() - 1)
    slot = jnp.sum(
        jnp.where(row_mask, per_token + (owner * slots).astype(F32), F32(0.0)),
        axis=0,
        keepdims=True,
    )
    slot_ref[...] = jnp.zeros(slot_ref.shape, F32)
    for k in range(codes.shape[0]):
        slot_ref[k : k + 1, :] = slot[:, k * LANES : (k + 1) * LANES]
    fetch_tokens.wait()


def serve_kernel(pay_ref, book_ref, send_ref, rank_ref, counts_ref, ent_ref, least_ref, near_ref, sem, *, slots, total_tokens):
    fetch = pltpu.make_async_copy(book_ref, near_ref, sem)
    fetch.start()
    per_dev = book_ref.shape[0]
    tiles = counts_ref.shape[0]
    span = per_dev // tiles
    devices = pay_ref.shape[0] // tiles
    coded = pay_ref[...]
    least_ref[0, 0] = jnp.min(coded)
    hist = jnp.where(coded < 0.0, -1.0 - coded, coded)
    present = hist > 0.5
    rank_ref[...] = jnp.where(present, rank_within(present, tiles)[0], F32(-1.0))
    fetch.wait()
    book = near_ref[...]
    steps = iota((slots, LANES), 0).astype(F32)

    def group(g, carry):
        ranks = rank_ref[pl.ds(pl.multiple_of(g * 8 * tiles, 8), 8 * tiles), :]
        pick = jnp.concatenate(
            [
                jnp.concatenate(
                    [
                        ones_where(steps == ranks[i * tiles + j : i * tiles + j + 1, :])
                        for j in range(tiles)
                    ],
                    axis=1,
                )
                for i in range(8)
            ],
            axis=0,
        )
        rows = dot(pick[:, :per_dev], book).astype(BF16)
        send_ref[pl.ds(pl.multiple_of(g * 8 * slots, 8 * slots), 8 * slots), :] = rows
        return carry

    lax.fori_loop(0, devices // 8, group, 0, unroll=True if devices <= 32 else 1)
    counts = fold(hist, tiles)
    counts_ref[...] = counts[:, :span].astype(jnp.int32)
    probs = counts / total_tokens
    terms = jnp.where(
        counts > 0.5,
        probs * jnp.log(jnp.maximum(probs, F32(1.0 / total_tokens))),
        F32(0.0),
    )
    ent = jnp.sum(jnp.sum(terms, axis=1, keepdims=True), axis=0, keepdims=True)
    ent_ref[...] = jnp.broadcast_to(ent, ent_ref.shape)


def loss_kernel(slot_ref, tokens_ref, recv_ref, ent_ref, quant_ref, loss_ref, back_ref, near_ref, sems, *, slots, block):
    tok_rows, width = tokens_ref.shape
    chunks = tok_rows // LANES
    devices = back_ref.shape[0]
    slot = slot_ref[...]
    cols = slot.T
    steps = iota((LANES, block), 1).astype(F32)
    copies = []
    lane = iota((LANES, LANES), 1)
    losses = jnp.zeros((LANES, LANES), F32)
    per_half = chunks // 2
    for half in range(2):
        at = pl.ds(half * per_half * LANES, per_half * LANES)
        near = range(half * per_half, (half + 1) * per_half)

        def pick(first):
            return jnp.concatenate(
                [ones_where(steps == cols[:, k : k + 1] - first) for k in near], axis=0
            )

        if recv_ref.shape[0] == block:
            quant = dot(pick(F32(0.0)), recv_ref[...])
        else:

            def gather(b, acc):
                start = pl.multiple_of(b * block, block)
                return acc + dot(pick((b * block).astype(F32)), recv_ref[pl.ds(start, block), :])

            quant = lax.fori_loop(
                0,
                recv_ref.shape[0] // block,
                gather,
                jnp.zeros((per_half * LANES, width), F32),
            )
        near_ref[at, :] = quant.astype(BF16)
        copy = pltpu.make_async_copy(near_ref.at[at, :], quant_ref.at[at, :], sems.at[half])
        copy.start()
        copies.append(copy)
        diff = tokens_ref[at, :].astype(F32) - quant
        loss = jnp.sum(diff * diff, axis=1, keepdims=True) / width
        for i, k in enumerate(near):
            losses = jnp.where(lane == k, loss[i * LANES : (i + 1) * LANES, :], losses)
    turned = losses.T
    loss_ref[...] = turned[:chunks, :]
    loss_row = jnp.concatenate([turned[k : k + 1, :] for k in range(chunks)], axis=1)
    total = jnp.sum(loss_row, axis=1, keepdims=True)
    slot_int = slot.astype(jnp.int32)[:chunks]
    shift = slots.bit_length() - 1
    owner_mask = rows_equal(slot_int >> shift, devices)
    rank = ones_where(rows_equal(slot_int & (slots - 1), LANES))
    high = loss_row.astype(BF16).astype(F32)
    mid = (loss_row - high).astype(BF16).astype(F32)
    low = loss_row - high - mid
    weighted = jnp.concatenate(
        [jnp.where(owner_mask, p, F32(0.0)).astype(BF16) for p in (low, mid, high)],
        axis=1,
    )
    sums = dot(weighted, jnp.concatenate([rank] * 3, axis=1), ((1,), (1,)))
    lane = iota((devices, LANES), 1)
    ent = jnp.broadcast_to(ent_ref[...], (devices, LANES))
    back_ref[...] = jnp.where(
        lane == slots, total, jnp.where(lane == slots + 1, ent, sums)
    )
    for copy in copies:
        copy.wait()


def collect_kernel(back_ref, rank_ref, code_loss_ref, commit_ref, perp_ref, *, slots, total_tokens):
    devices = back_ref.shape[0]
    tiles = code_loss_ref.shape[0]
    back = back_ref[...]
    high = back.astype(BF16).astype(F32)
    mid = (back - high).astype(BF16).astype(F32)
    parts = jnp.concatenate(
        [p.astype(BF16) for p in (back - high - mid, mid, high)], axis=0
    )
    shape = (devices * tiles, devices)
    repeat = ones_where((iota(shape, 0) >> (tiles.bit_length() - 1)) == iota(shape, 1))
    spread = dot(jnp.concatenate([repeat] * 3, axis=1), parts)
    rank = rank_ref[...].astype(jnp.int32)
    found = jnp.take_along_axis(spread, jnp.maximum(rank, 0), axis=1)
    code_loss = fold(jnp.where(rank >= 0, found, F32(0.0)), tiles)
    code_loss_ref[...] = code_loss[:, : code_loss_ref.shape[1]]
    sums = jnp.sum(back_ref[...], axis=0, keepdims=True)
    commit_ref[...] = 0.25 * sums[:, slots : slots + 1] / total_tokens
    perp_ref[...] = jnp.exp(-sums[:, slots + 1 : slots + 2])


def on_device(tokens, codebook, codes, *, devices):
    tok_rows, width = tokens.shape
    per_dev = codebook.shape[0]
    total_tokens = tok_rows * devices
    slots = min(SLOTS, per_dev)
    chunks = tok_rows // LANES
    n_slots = devices * slots
    shape = jax.ShapeDtypeStruct

    tiles = max(per_dev // LANES, 1)
    pay, slot, near_tokens = pl.pallas_call(
        functools.partial(request_kernel, devices=devices, per_dev=per_dev, slots=slots),
        out_shape=(
            shape((devices * tiles, LANES), F32),
            shape((-(-chunks // 8) * 8, LANES), F32),
            shape(tokens.shape, BF16),
        ),
        in_specs=[VMEM, ANY],
        out_specs=(VMEM,) * 3,
        scratch_shapes=[pltpu.SemaphoreType.DMA],
        name="request",
    )(codes.reshape(chunks, LANES), tokens)
    pay_in = lax.all_to_all(pay.reshape(devices, tiles, LANES), AXES, 0, 0)
    pay_in = pay_in.reshape(devices * tiles, LANES)
    send, rank, counts, ent, least = pl.pallas_call(
        functools.partial(serve_kernel, slots=slots, total_tokens=total_tokens),
        out_shape=(
            shape((n_slots, width), BF16),
            shape((devices * tiles, LANES), F32),
            shape((tiles, per_dev // tiles), jnp.int32),
            shape((1, LANES), F32),
            shape((1, 1), F32),
        ),
        in_specs=[VMEM, ANY],
        out_specs=(VMEM, VMEM, VMEM, VMEM, SMEM),
        scratch_shapes=[pltpu.VMEM(codebook.shape, BF16), pltpu.SemaphoreType.DMA],
        name="serve",
    )(pay_in, codebook)
    code_counts = counts.reshape(per_dev)

    def exchange_slots(tokens, near_tokens, codebook, codes, slot, send, rank, ent):
        recv = lax.all_to_all(send, AXES, 0, 0, tiled=True)
        quantized, loss, back = pl.pallas_call(
            functools.partial(loss_kernel, slots=slots, block=min(n_slots, 1024)),
            out_shape=(
                shape((tok_rows, width), BF16),
                shape((chunks, LANES), F32),
                shape((devices, LANES), F32),
            ),
            in_specs=[VMEM] * 4,
            out_specs=(ANY, VMEM, VMEM),
            scratch_shapes=[
                pltpu.VMEM((tok_rows, width), BF16),
                pltpu.SemaphoreType.DMA((2,)),
            ],
            name="losses",
        )(slot, near_tokens, recv, ent)
        back_in = lax.all_to_all(back, AXES, 0, 0, tiled=True)
        code_loss, commit, perp = pl.pallas_call(
            functools.partial(collect_kernel, slots=slots, total_tokens=total_tokens),
            out_shape=(shape((tiles, per_dev // tiles), F32), shape((1, 1), F32), shape((1, 1), F32)),
            in_specs=[VMEM] * 2,
            out_specs=(VMEM,) * 3,
            name="collect",
        )(back_in, rank)
        return (
            quantized,
            loss.reshape(tok_rows),
            code_loss.reshape(per_dev),
            commit.reshape(()),
            perp.reshape(()),
        )

    def exchange_book(tokens, near_tokens, codebook, codes, slot, send, rank, ent):
        spread = jnp.broadcast_to(codebook[None], (devices, per_dev, width))
        book = lax.all_to_all(spread, AXES, 0, 0, tiled=True)
        book = book.reshape(devices * per_dev, width)
        quantized = jnp.take(book, codes, axis=0, mode="clip")
        diff = tokens.astype(F32) - quantized.astype(F32)
        token_loss = jnp.sum(diff * diff, axis=1) / width
        part = jax.ops.segment_sum(token_loss, codes, num_segments=devices * per_dev)
        part = lax.all_to_all(part.reshape(devices, per_dev), AXES, 0, 0, tiled=True)
        lane = iota((devices, LANES), 1)
        pair = jnp.where(lane == 0, jnp.sum(token_loss), ent)
        sums = jnp.sum(lax.all_to_all(pair, AXES, 0, 0, tiled=True), axis=0)
        return (
            quantized,
            token_loss,
            jnp.sum(part, axis=0),
            0.25 * sums[0] / total_tokens,
            jnp.exp(-sums[1]),
        )

    quantized, token_loss, code_loss, commitment, perplexity = lax.cond(
        least[0, 0] < 0.0,
        exchange_book,
        exchange_slots,
        tokens, near_tokens, codebook, codes, slot, send, rank, ent,
    )
    return (quantized, token_loss, code_counts, code_loss, commitment, perplexity)


def solution(mesh):
    devices = mesh.shape["row"] * mesh.shape["col"]
    split = P(AXES)
    return jax.shard_map(
        functools.partial(on_device, devices=devices),
        mesh=mesh,
        in_specs=(P(AXES, None), P(AXES, None), split),
        out_specs=(P(AXES, None), split, split, split, P(), P()),
        check_vma=False,
    )
```

```python
import functools

import jax
import jax.numpy as jnp
from jax import lax
from jax.experimental import pallas as pl
from jax.experimental.pallas import tpu as pltpu
from jax.sharding import PartitionSpec as P

AXES = ("row", "col")
LANES = 128
SLOTS = 32
F32 = jnp.float32
BF16 = jnp.bfloat16
VMEM = pl.BlockSpec(memory_space=pltpu.VMEM)
ANY = pl.BlockSpec(memory_space=pl.ANY)
SMEM = pl.BlockSpec(memory_space=pltpu.SMEM)


def iota(shape, dim):
    return lax.broadcasted_iota(jnp.int32, shape, dim)


def ones_where(mask):
    return jnp.where(mask, F32(1.0), F32(0.0)).astype(BF16)


def dot(a, b, dims=((1,), (0,))):
    return lax.dot_general(a, b, (dims, ((), ())), preferred_element_type=F32)


def fold(x, rows):
    while x.shape[0] > rows:
        half = x.shape[0] // 2
        x = x[:half] + x[half:]
    return x


def rank_within(present, tiles):
    ones = ones_where(present)
    lane = (LANES, LANES)
    rank = dot(ones, ones_where(iota(lane, 0) < iota(lane, 1)))
    unique = jnp.sum(jnp.where(present, F32(1.0), F32(0.0)), axis=1, keepdims=True)
    row = iota(unique.shape, 0) & (tiles - 1)
    earlier = jnp.zeros_like(unique)
    for j in range(1, tiles):
        moved = pltpu.roll(jnp.broadcast_to(unique, present.shape), j, 0)[:, :1]
        earlier = earlier + jnp.where(row >= j, moved, F32(0.0))
    return rank + earlier, unique + earlier


def rows_equal(ids, count):
    steps = iota((count, LANES), 0)
    return jnp.concatenate(
        [steps == ids[k : k + 1, :] for k in range(ids.shape[0])], axis=1
    )


def request_kernel(codes_ref, pay_ref, slot_ref, *, devices, per_dev, slots):
    codes = codes_ref[...]
    tiles = pay_ref.shape[0] // devices
    span = per_dev // tiles
    row_mask = rows_equal(codes >> (span.bit_length() - 1), devices * tiles)
    lanes = ones_where(rows_equal(codes & (span - 1), LANES))
    hist = dot(ones_where(row_mask), lanes, ((1,), (1,)))
    rank, unique = rank_within(hist > 0.5, tiles)
    most = jnp.max(unique, axis=0, keepdims=True)
    pay_ref[...] = jnp.where(most > F32(slots), -1.0 - hist, hist)
    capped = jnp.minimum(rank, F32(slots - 1)).astype(BF16)
    per_token = dot(capped, lanes)
    owner = iota(row_mask.shape, 0) >> (tiles.bit_length() - 1)
    slot = jnp.sum(
        jnp.where(row_mask, per_token + (owner * slots).astype(F32), F32(0.0)),
        axis=0,
        keepdims=True,
    )
    slot_ref[...] = jnp.zeros(slot_ref.shape, F32)
    for k in range(codes.shape[0]):
        slot_ref[k : k + 1, :] = slot[:, k * LANES : (k + 1) * LANES]


def serve_kernel(pay_ref, book_ref, send_ref, rank_ref, counts_ref, ent_ref, least_ref, near_ref, sem, *, slots, total_tokens):
    fetch = pltpu.make_async_copy(book_ref, near_ref, sem)
    fetch.start()
    per_dev = book_ref.shape[0]
    tiles = counts_ref.shape[0]
    span = per_dev // tiles
    devices = pay_ref.shape[0] // tiles
    coded = pay_ref[...]
    least_ref[0, 0] = jnp.min(coded)
    hist = jnp.where(coded < 0.0, -1.0 - coded, coded)
    present = hist > 0.5
    rank_ref[...] = jnp.where(present, rank_within(present, tiles)[0], F32(-1.0))
    fetch.wait()
    book = near_ref[...]
    steps = iota((slots, LANES), 0).astype(F32)

    def group(g, carry):
        ranks = rank_ref[pl.ds(pl.multiple_of(g * 8 * tiles, 8), 8 * tiles), :]
        pick = jnp.concatenate(
            [
                jnp.concatenate(
                    [
                        ones_where(steps == ranks[i * tiles + j : i * tiles + j + 1, :])
                        for j in range(tiles)
                    ],
                    axis=1,
                )
                for i in range(8)
            ],
            axis=0,
        )
        rows = dot(pick[:, :per_dev], book).astype(BF16)
        send_ref[pl.ds(pl.multiple_of(g * 8 * slots, 8 * slots), 8 * slots), :] = rows
        return carry

    lax.fori_loop(0, devices // 8, group, 0, unroll=True if devices <= 32 else 1)
    counts = fold(hist, tiles)
    counts_ref[...] = counts[:, :span].astype(jnp.int32)
    probs = counts / total_tokens
    terms = jnp.where(
        counts > 0.5,
        probs * jnp.log(jnp.maximum(probs, F32(1.0 / total_tokens))),
        F32(0.0),
    )
    ent = jnp.sum(jnp.sum(terms, axis=1, keepdims=True), axis=0, keepdims=True)
    ent_ref[...] = jnp.broadcast_to(ent, ent_ref.shape)


def loss_kernel(slot_ref, tokens_ref, recv_ref, ent_ref, quant_ref, loss_ref, back_ref, near_ref, near_tokens_ref, sems, *, slots, block):
    fetch = pltpu.make_async_copy(tokens_ref, near_tokens_ref, sems.at[2])
    fetch.start()
    tok_rows, width = tokens_ref.shape
    chunks = tok_rows // LANES
    devices = back_ref.shape[0]
    slot = slot_ref[...]
    cols = slot.T
    steps = iota((LANES, block), 1).astype(F32)
    copies = []
    lane = iota((LANES, LANES), 1)
    losses = jnp.zeros((LANES, LANES), F32)
    per_half = chunks // 2
    for half in range(2):
        at = pl.ds(half * per_half * LANES, per_half * LANES)
        near = range(half * per_half, (half + 1) * per_half)

        def pick(first):
            return jnp.concatenate(
                [ones_where(steps == cols[:, k : k + 1] - first) for k in near], axis=0
            )

        if recv_ref.shape[0] == block:
            quant = dot(pick(F32(0.0)), recv_ref[...])
        else:

            def gather(b, acc):
                start = pl.multiple_of(b * block, block)
                return acc + dot(pick((b * block).astype(F32)), recv_ref[pl.ds(start, block), :])

            quant = lax.fori_loop(
                0,
                recv_ref.shape[0] // block,
                gather,
                jnp.zeros((per_half * LANES, width), F32),
            )
        near_ref[at, :] = quant.astype(BF16)
        copy = pltpu.make_async_copy(near_ref.at[at, :], quant_ref.at[at, :], sems.at[half])
        copy.start()
        copies.append(copy)
        if half == 0:
            fetch.wait()
        diff = near_tokens_ref[at, :].astype(F32) - quant
        loss = jnp.sum(diff * diff, axis=1, keepdims=True) / width
        for i, k in enumerate(near):
            losses = jnp.where(lane == k, loss[i * LANES : (i + 1) * LANES, :], losses)
    turned = losses.T
    loss_ref[...] = turned[:chunks, :]
    loss_row = jnp.concatenate([turned[k : k + 1, :] for k in range(chunks)], axis=1)
    total = jnp.sum(loss_row, axis=1, keepdims=True)
    slot_int = slot.astype(jnp.int32)[:chunks]
    shift = slots.bit_length() - 1
    owner_mask = rows_equal(slot_int >> shift, devices)
    rank = ones_where(rows_equal(slot_int & (slots - 1), LANES))
    high = loss_row.astype(BF16).astype(F32)
    mid = (loss_row - high).astype(BF16).astype(F32)
    low = loss_row - high - mid
    weighted = jnp.concatenate(
        [jnp.where(owner_mask, p, F32(0.0)).astype(BF16) for p in (low, mid, high)],
        axis=1,
    )
    sums = dot(weighted, jnp.concatenate([rank] * 3, axis=1), ((1,), (1,)))
    lane = iota((devices, LANES), 1)
    ent = jnp.broadcast_to(ent_ref[...], (devices, LANES))
    back_ref[...] = jnp.where(
        lane == slots, total, jnp.where(lane == slots + 1, ent, sums)
    )
    for copy in copies:
        copy.wait()


def collect_kernel(back_ref, rank_ref, code_loss_ref, commit_ref, perp_ref, *, slots, total_tokens):
    devices = back_ref.shape[0]
    tiles = code_loss_ref.shape[0]
    back = back_ref[...]
    high = back.astype(BF16).astype(F32)
    mid = (back - high).astype(BF16).astype(F32)
    parts = jnp.concatenate(
        [p.astype(BF16) for p in (back - high - mid, mid, high)], axis=0
    )
    shape = (devices * tiles, devices)
    repeat = ones_where((iota(shape, 0) >> (tiles.bit_length() - 1)) == iota(shape, 1))
    spread = dot(jnp.concatenate([repeat] * 3, axis=1), parts)
    rank = rank_ref[...].astype(jnp.int32)
    found = jnp.take_along_axis(spread, jnp.maximum(rank, 0), axis=1)
    code_loss = fold(jnp.where(rank >= 0, found, F32(0.0)), tiles)
    code_loss_ref[...] = code_loss[:, : code_loss_ref.shape[1]]
    sums = jnp.sum(back_ref[...], axis=0, keepdims=True)
    commit_ref[...] = 0.25 * sums[:, slots : slots + 1] / total_tokens
    perp_ref[...] = jnp.exp(-sums[:, slots + 1 : slots + 2])


def on_device(tokens, codebook, codes, *, devices):
    tok_rows, width = tokens.shape
    per_dev = codebook.shape[0]
    total_tokens = tok_rows * devices
    slots = min(SLOTS, per_dev)
    chunks = tok_rows // LANES
    n_slots = devices * slots
    shape = jax.ShapeDtypeStruct

    tiles = max(per_dev // LANES, 1)
    pay, slot = pl.pallas_call(
        functools.partial(request_kernel, devices=devices, per_dev=per_dev, slots=slots),
        out_shape=(
            shape((devices * tiles, LANES), F32),
            shape((-(-chunks // 8) * 8, LANES), F32),
        ),
        in_specs=[VMEM],
        out_specs=(VMEM,) * 2,
        name="request",
    )(codes.reshape(chunks, LANES))
    pay_in = lax.all_to_all(pay.reshape(devices, tiles, LANES), AXES, 0, 0)
    pay_in = pay_in.reshape(devices * tiles, LANES)
    send, rank, counts, ent, least = pl.pallas_call(
        functools.partial(serve_kernel, slots=slots, total_tokens=total_tokens),
        out_shape=(
            shape((n_slots, width), BF16),
            shape((devices * tiles, LANES), F32),
            shape((tiles, per_dev // tiles), jnp.int32),
            shape((1, LANES), F32),
            shape((1, 1), F32),
        ),
        in_specs=[VMEM, ANY],
        out_specs=(VMEM, VMEM, VMEM, VMEM, SMEM),
        scratch_shapes=[pltpu.VMEM(codebook.shape, BF16), pltpu.SemaphoreType.DMA],
        name="serve",
    )(pay_in, codebook)
    code_counts = counts.reshape(per_dev)

    def exchange_slots(tokens, codebook, codes, slot, send, rank, ent):
        recv = lax.all_to_all(send, AXES, 0, 0, tiled=True)
        quantized, loss, back = pl.pallas_call(
            functools.partial(loss_kernel, slots=slots, block=min(n_slots, 1024)),
            out_shape=(
                shape((tok_rows, width), BF16),
                shape((chunks, LANES), F32),
                shape((devices, LANES), F32),
            ),
            in_specs=[VMEM, ANY, VMEM, VMEM],
            out_specs=(ANY, VMEM, VMEM),
            scratch_shapes=[
                pltpu.VMEM((tok_rows, width), BF16),
                pltpu.VMEM((tok_rows, width), BF16),
                pltpu.SemaphoreType.DMA((3,)),
            ],
            name="losses",
        )(slot, tokens, recv, ent)
        back_in = lax.all_to_all(back, AXES, 0, 0, tiled=True)
        code_loss, commit, perp = pl.pallas_call(
            functools.partial(collect_kernel, slots=slots, total_tokens=total_tokens),
            out_shape=(shape((tiles, per_dev // tiles), F32), shape((1, 1), F32), shape((1, 1), F32)),
            in_specs=[VMEM] * 2,
            out_specs=(VMEM,) * 3,
            name="collect",
        )(back_in, rank)
        return (
            quantized,
            loss.reshape(tok_rows),
            code_loss.reshape(per_dev),
            commit.reshape(()),
            perp.reshape(()),
        )

    def exchange_book(tokens, codebook, codes, slot, send, rank, ent):
        spread = jnp.broadcast_to(codebook[None], (devices, per_dev, width))
        book = lax.all_to_all(spread, AXES, 0, 0, tiled=True)
        book = book.reshape(devices * per_dev, width)
        quantized = jnp.take(book, codes, axis=0, mode="clip")
        diff = tokens.astype(F32) - quantized.astype(F32)
        token_loss = jnp.sum(diff * diff, axis=1) / width
        part = jax.ops.segment_sum(token_loss, codes, num_segments=devices * per_dev)
        part = lax.all_to_all(part.reshape(devices, per_dev), AXES, 0, 0, tiled=True)
        lane = iota((devices, LANES), 1)
        pair = jnp.where(lane == 0, jnp.sum(token_loss), ent)
        sums = jnp.sum(lax.all_to_all(pair, AXES, 0, 0, tiled=True), axis=0)
        return (
            quantized,
            token_loss,
            jnp.sum(part, axis=0),
            0.25 * sums[0] / total_tokens,
            jnp.exp(-sums[1]),
        )

    quantized, token_loss, code_loss, commitment, perplexity = lax.cond(
        least[0, 0] < 0.0,
        exchange_book,
        exchange_slots,
        tokens, codebook, codes, slot, send, rank, ent,
    )
    return (quantized, token_loss, code_counts, code_loss, commitment, perplexity)


def solution(mesh):
    devices = mesh.shape["row"] * mesh.shape["col"]
    split = P(AXES)
    return jax.shard_map(
        functools.partial(on_device, devices=devices),
        mesh=mesh,
        in_specs=(P(AXES, None), P(AXES, None), split),
        out_specs=(P(AXES, None), split, split, split, P(), P()),
        check_vma=False,
    )
```
